32 devices in a mesh: replica: 4 (over x, core), fsdp: 8 (over z, y).
Axes of the slice: x: 2, y: 2, z: 4, core: 2. Of those that a mesh axis runs over, the one named last changes fastest.
Arguments:
- deltas: bfloat16 [4, 2, 2048, 16384], P('replica', None, 'fsdp'), may hold values from -3 to 3
- master: float32 [2, 2048, 16384], P(None, 'replica', 'fsdp'), may hold values from -3 to 3
- momentum: float32 [2, 2048, 16384], P(None, 'replica', 'fsdp'), may hold values from -2 to 2
Outputs:
- master_out: float32 [2, 2048, 16384], P(None, 'replica', 'fsdp')
- momentum_out: float32 [2, 2048, 16384], P(None, 'replica', 'fsdp')
- params_out: bfloat16 [2, 2048, 16384], P(None, 'fsdp')
The draws below stay inside these ranges and needn't reach their ends.
All inputs are finite; a program needn't handle non-finite values.
Results may differ from the reference program's by a relative error of at most 0.008.
Values may be sent and summed in bfloat16 or wider, within the bound.
A program may use at most 128 MiB of HBM per device.

```python
import jax
import jax.numpy as jnp

D = 2048
FF = 16384
PROJ = 2
R = 4


def strengthened(result, own_key, source, target, shards_of, factor):
    def block_of(dim):
        return (jnp.arange(result.shape[dim]) // (result.shape[dim] // shards_of)).reshape((-1,) + (1,) * (result.ndim - 1 - dim))

    one_side = jax.random.permutation(own_key, shards_of)[block_of(target)]
    other_side = (block_of(target) + shards_of // 2) % shards_of
    return jnp.where((block_of(source) == one_side) | (block_of(source) == other_side), factor * result, result)


def steps_of(rng, dims, shards, low, high):
    factor_of, own = 1.0, jax.random.fold_in(rng, 6)
    for dim, blocks in shards:
        steps = jnp.exp(jax.random.uniform(jax.random.fold_in(own, dim), (blocks,), jnp.float32, low / len(shards), high / len(shards)))
        factor_of = factor_of * jnp.repeat(steps, dims[dim] // blocks).reshape([-1 if axis == dim else 1 for axis in range(len(dims))])
    return factor_of


def normal_values(rng, dims, scale, limit, split=(), kind=jnp.bfloat16):
    drawn = jax.random.normal(rng, dims, jnp.float32) * scale
    if len(split) > 0:
        drawn = steps_of(rng, dims, split, -0.22, 0.18) * drawn
    return jnp.clip(drawn, min=-limit, max=limit).astype(kind)


def heavy_noise(rng, shape, spread, most, split, heavy, held_as=jnp.bfloat16):
    values = spread * jax.random.normal(rng, shape, jnp.float32)
    if split:
        values = values * steps_of(rng, shape, split, -0.22, 0.18)
    return jnp.clip(strengthened(values, jax.random.fold_in(rng, 3), *heavy), -most, most).astype(held_as)


def setup_inputs(seed: int = 0) -> dict:
    splits = jax.random.split(jax.random.key(seed), 4)
    deltas = heavy_noise(splits[0], (R, PROJ, D, FF), 0.5, 3.0, ((0, 4), (2, 8)), (0, 2, 4, 2.0))
    master = normal_values(splits[1], (PROJ, D, FF), 0.5, 3.0, ((1, 4), (2, 8)), jnp.float32)
    momentum = normal_values(splits[2], (PROJ, D, FF), 0.3, 2.0, ((1, 4), (2, 8)), jnp.float32)
    return {"deltas": deltas, "master": master, "momentum": momentum}


def reference(deltas, master, momentum):
    outer = jnp.sum(deltas.astype(jnp.float32), axis=0) / deltas.shape[0]
    velocity = 0.9 * momentum + outer
    updated = master - 0.7 * (outer + 0.9 * velocity)
    return updated, velocity, updated.astype(jnp.bfloat16)
```

```python
import functools

import jax
import jax.numpy as jnp
from jax import lax
from jax.experimental import pallas as pl
from jax.experimental.pallas import tpu as pltpu
from jax.sharding import PartitionSpec as P

F32, BF16 = jnp.float32, jnp.bfloat16
SPLITS = 16
AHEAD = 8
LAGS = (4, 8, 12, 15)


def kernel(
    dims, delta, master, momentum, mas, mom, out,
    half, cross, total,
    load, load_own, sent, pair_in, cross_in, total_in, back_in, side_in, last_in,
):
    R, F, PROJ, RB, FF, WD, H = dims
    B, S, T = F // R, RB // H, F * H
    w, f = lax.axis_index("replica"), lax.axis_index("fsdp")
    core, x = lax.rem(w, PROJ), w // PROJ
    a, b = f // B, lax.rem(f, B)
    other = 1 - core
    pair = (x * PROJ + other, f)
    side = ((1 - x) * PROJ + core, f)
    near = x == a // PROJ
    far = jnp.logical_not(near)
    mine = a == w

    def to(ref_src, ref_dst, send, recv, device):
        return pltpu.make_async_remote_copy(
            src_ref=ref_src, dst_ref=ref_dst, send_sem=send, recv_sem=recv,
            device_id=device, device_id_type=pl.DeviceIdType.MESH,
        )

    def drain(ref, sem):
        pltpu.make_async_copy(ref, ref, sem).wait()

    def block(c, t):
        return lax.rem(lax.rem(t, F) + f + c * (F // 2), F)

    def rows(t):
        return pl.ds(pl.multiple_of((t // F) * S, S), S)

    def cols(i):
        return pl.ds(pl.multiple_of(i * WD, 128), WD)

    def own_rows(h):
        r = pl.ds(pl.multiple_of(h * S, S), S)
        return pltpu.make_async_copy(delta.at[core, r], out.at[core, r], load_own.at[h])

    barrier = pltpu.get_barrier_semaphore()

    def greet(device):
        pl.semaphore_signal(barrier, inc=1, device_id=device, device_id_type=pl.DeviceIdType.MESH)

    greet(pair)
    greet(side)

    @pl.loop(0, PROJ * B)
    def _(i):
        p, bi = i // B, lax.rem(i, B)

        @pl.when(jnp.logical_not(jnp.logical_and(mine, jnp.logical_and(p == core, bi == b))))
        def _():
            greet((x * PROJ + p, w * B + bi))

    @pl.when(near)
    def _():
        @pl.loop(0, F)
        def _(i):
            @pl.when(jnp.logical_not(jnp.logical_and(mine, i == f)))
            def _():
                greet((a, i))

    @pl.loop(0, H)
    def _(h):
        own_rows(h).start()

    @pl.when(far)
    def _():
        pl.semaphore_wait(barrier, 2 + PROJ * B)

    @pl.when(mine)
    def _():
        pl.semaphore_wait(barrier, PROJ * B + F)

    @pl.when(jnp.logical_and(near, jnp.logical_not(mine)))
    def _():
        pl.semaphore_wait(barrier, 2 + PROJ * B + F)

    def send_pair(t):
        c = cols(block(other, t))
        to(delta.at[other, rows(t), c], half.at[rows(t), c], sent.at[0], pair_in.at[t], pair).start()

    def step_cross(t):
        @pl.when(lax.rem(t, F) == 0)
        def _():
            own_rows(t // F).wait()

        r, c = rows(t), cols(block(core, t))
        tile = half.at[r, c]
        pltpu.make_async_copy(tile, tile, pair_in.at[t]).wait()
        tile[...] = (tile[...].astype(F32) + out[core, r, c].astype(F32)).astype(BF16)
        to(tile, cross.at[r, c], sent.at[1], cross_in.at[t], side).start()

    def slot(p, bi, h):
        return total.at[p, pl.ds(pl.multiple_of(bi * RB + h * S, S), S)]

    def step_total(t):
        h = t // F

        @pl.when(lax.rem(t, F) == 0)
        def _():
            own_rows(h).wait()

        i = block(core, t)
        r, c = rows(t), cols(i)
        tile, arrived = half.at[r, c], cross.at[r, c]
        pltpu.make_async_copy(tile, tile, pair_in.at[t]).wait()
        pltpu.make_async_copy(arrived, arrived, cross_in.at[t]).wait()
        tile[...] = (
            tile[...].astype(F32) + out[core, r, c].astype(F32) + arrived[...].astype(F32)
        ).astype(BF16)
        dst, sem = slot(core, b, h), total_in.at[(core * B + b) * H + h]
        here = jnp.logical_and(mine, i == f)

        @pl.when(here)
        def _():
            pltpu.make_async_copy(tile, dst, sem).start()

        @pl.when(jnp.logical_not(here))
        def _():
            to(tile, dst, sent.at[2], sem, (a, i)).start()

    def step_update(t):
        h, k = t // F, lax.rem(t, F)
        for p in range(PROJ):
            e = lax.rem(f + 2 * F - k - p * (F // 2), F)

            @pl.when(e // B == w)
            def _():
                be = lax.rem(e, B)
                tile = slot(p, be, h)
                pltpu.make_async_copy(tile, tile, total_in.at[(p * B + be) * H + h]).wait()
                rr = pl.ds(pl.multiple_of(be * RB + h * S, S), S)
                outer = tile[...].astype(F32) / R
                velocity = 0.9 * mom[p, rr] + outer
                updated = mas[p, rr] - 0.7 * (outer + 0.9 * velocity)
                mom[p, rr] = velocity
                mas[p, rr] = updated
                tile[...] = updated.astype(BF16)
                dst = out.at[p, rows(t), cols(f)]
                here = jnp.logical_and(mine, jnp.logical_and(p == core, e == f))

                @pl.when(here)
                def _():
                    pltpu.make_async_copy(tile, dst, back_in.at[t]).start()

                @pl.when(jnp.logical_not(here))
                def _():
                    to(tile, dst, sent.at[3], back_in.at[t], (x * PROJ + p, e)).start()

    def step_side(t):
        tile = out.at[core, rows(t), cols(block(core, t))]
        pltpu.make_async_copy(tile, tile, back_in.at[t]).wait()
        to(tile, tile, sent.at[4], side_in.at[t], side).start()
        to(tile, tile, sent.at[5], last_in, pair).start()

    def step_pair(t):
        tile = out.at[core, rows(t), cols(block(core, t))]
        pltpu.make_async_copy(tile, tile, side_in.at[t]).wait()
        to(tile, tile, sent.at[5], last_in, pair).start()

    @pl.loop(0, min(AHEAD, T))
    def _(t):
        send_pair(t)

    load_mas = pltpu.make_async_copy(master, mas, load.at[0])
    load_mom = pltpu.make_async_copy(momentum, mom, load.at[1])

    @pl.loop(0, T + LAGS[-1])
    def _(t):
        @pl.when(t + AHEAD < T)
        def _():
            send_pair(t + AHEAD)

        @pl.when(jnp.logical_and(far, t < T))
        def _():
            step_cross(t)

        @pl.when(t == 0)
        def _():
            load_mas.start()
            load_mom.start()

        @pl.when(t == LAGS[1])
        def _():
            load_mas.wait()
            load_mom.wait()

        def late(lag, on, step):
            @pl.when(jnp.logical_and(on, jnp.logical_and(t >= lag, t < T + lag)))
            def _():
                step(t - lag)

        late(LAGS[0], near, step_total)
        late(LAGS[1], True, step_update)
        late(LAGS[2], near, step_side)
        late(LAGS[3], far, step_pair)

    drain(out.at[other], last_in)
    drain(half, sent.at[0])
    drain(half, sent.at[5])

    def drain_blocks(n, sem):
        drain(half.at[pl.ds(0, RB), pl.ds(0, n * WD)], sem)

    @pl.when(far)
    def _():
        drain_blocks(F, sent.at[1])
        drain_blocks(PROJ * B, sent.at[3])

    @pl.when(near)
    def _():
        drain_blocks(F, sent.at[4])

    @pl.when(mine)
    def _():
        drain_blocks(F - 1, sent.at[2])
        drain_blocks(PROJ * B - 1, sent.at[3])

    @pl.when(jnp.logical_and(near, jnp.logical_not(mine)))
    def _():
        drain_blocks(F, sent.at[2])
        drain_blocks(PROJ * B, sent.at[3])


def on_device(deltas, master, momentum):
    local = deltas[0]
    R, F = lax.axis_size("replica"), lax.axis_size("fsdp")
    PROJ, RB, FF = local.shape
    WD = FF // F
    H = min(SPLITS, RB // 16)
    assert R == 2 * PROJ and PROJ == 2 and F % R == 0 and RB % H == 0 and WD % 128 == 0
    T, B = F * H, F // R
    hbm, vmem = pl.BlockSpec(memory_space=pl.ANY), pl.BlockSpec(memory_space=pltpu.VMEM)
    dma = pltpu.SemaphoreType.DMA
    results = pl.pallas_call(
        functools.partial(kernel, (R, F, PROJ, RB, FF, WD, H)),
        out_shape=(
            pltpu.VMEM(master.shape, F32),
            pltpu.VMEM(momentum.shape, F32),
            pltpu.VMEM(local.shape, BF16),
        ),
        in_specs=[hbm] * 3,
        out_specs=(vmem,) * 3,
        scratch_shapes=[
            pltpu.VMEM((RB, FF), BF16),
            pltpu.VMEM((RB, FF), BF16),
            pltpu.VMEM(master.shape, BF16),
            dma((2,)), dma((H,)), dma((6,)),
            dma((T,)), dma((T,)), dma((PROJ * B * H,)), dma((T,)), dma((T,)), dma,
        ],
        compiler_params=pltpu.CompilerParams(
            collective_id=0, has_side_effects=True, vmem_limit_bytes=24 * 2**20
        ),
    )(local, master, momentum)
    return results


def solution(mesh):
    return jax.shard_map(
        on_device,
        mesh=mesh,
        in_specs=(
            P("replica", None, "fsdp", None),
            P(None, "replica", "fsdp"),
            P(None, "replica", "fsdp"),
        ),
        out_specs=(P(None, "replica", "fsdp"), P(None, "replica", "fsdp"), P(None, "fsdp", None)),
        check_vma=False,
    )
```

```python
import functools

import jax
import jax.numpy as jnp
from jax import lax
from jax.experimental import pallas as pl
from jax.experimental.pallas import tpu as pltpu
from jax.sharding import PartitionSpec as P

F32, BF16 = jnp.float32, jnp.bfloat16
SPLITS = 16
AHEAD = 8
PIECES = 4
LAGS = (6, 10, 14, 18)


def kernel(
    dims, delta, master, momentum, mas, mom, out,
    half, cross, total, first,
    load, load_own, sent, pair_in, cross_in, total_in, back_in, side_in, last_in,
):
    R, F, PROJ, RB, FF, WD, H = dims
    B, S, T = F // R, RB // H, F * H
    w, f = lax.axis_index("replica"), lax.axis_index("fsdp")
    core, x = lax.rem(w, PROJ), w // PROJ
    a, b = f // B, lax.rem(f, B)
    other = 1 - core
    pair = (x * PROJ + other, f)
    side = ((1 - x) * PROJ + core, f)
    near = x == a // PROJ
    far = jnp.logical_not(near)
    mine = a == w

    def to(ref_src, ref_dst, send, recv, device):
        return pltpu.make_async_remote_copy(
            src_ref=ref_src, dst_ref=ref_dst, send_sem=send, recv_sem=recv,
            device_id=device, device_id_type=pl.DeviceIdType.MESH,
        )

    def drain(ref, sem):
        pltpu.make_async_copy(ref, ref, sem).wait()

    def block(c, t):
        return lax.rem(lax.rem(t, F) + f + c * (F // 2), F)

    def rows(t):
        return pl.ds(pl.multiple_of((t // F) * S, S), S)

    def cols(i):
        return pl.ds(pl.multiple_of(i * WD, 128), WD)

    def own_rows(h):
        r = pl.ds(pl.multiple_of(h * S, S), S)
        return pltpu.make_async_copy(delta.at[core, r], out.at[core, r], load_own.at[h])

    load_first = pltpu.make_async_copy(delta.at[other, pl.ds(0, S)], first, load.at[2])
    load_first.start()
    barrier = pltpu.get_barrier_semaphore()

    def greet(device):
        pl.semaphore_signal(barrier, inc=1, device_id=device, device_id_type=pl.DeviceIdType.MESH)

    greet(pair)
    greet(side)

    @pl.loop(0, PROJ * B)
    def _(i):
        p, bi = i // B, lax.rem(i, B)

        @pl.when(jnp.logical_not(jnp.logical_and(mine, jnp.logical_and(p == core, bi == b))))
        def _():
            greet((x * PROJ + p, w * B + bi))

    @pl.when(near)
    def _():
        @pl.loop(0, F)
        def _(i):
            @pl.when(jnp.logical_not(jnp.logical_and(mine, i == f)))
            def _():
                greet((a, i))

    @pl.loop(0, H)
    def _(h):
        own_rows(h).start()

    @pl.when(far)
    def _():
        pl.semaphore_wait(barrier, 2 + PROJ * B)

    @pl.when(mine)
    def _():
        pl.semaphore_wait(barrier, PROJ * B + F)

    @pl.when(jnp.logical_and(near, jnp.logical_not(mine)))
    def _():
        pl.semaphore_wait(barrier, 2 + PROJ * B + F)

    def send_pair(t):
        c = cols(block(other, t))
        dst, sem = half.at[rows(t), c], pair_in.at[t]

        @pl.when(t < F)
        def _():
            to(first.at[:, c], dst, sent.at[0], sem, pair).start()

        @pl.when(t >= F)
        def _():
            to(delta.at[other, rows(t), c], dst, sent.at[0], sem, pair).start()

    def step_cross(t):
        @pl.when(lax.rem(t, F) == 0)
        def _():
            own_rows(t // F).wait()

        r, c = rows(t), cols(block(core, t))
        tile = half.at[r, c]
        pltpu.make_async_copy(tile, tile, pair_in.at[t]).wait()
        tile[...] = (tile[...].astype(F32) + out[core, r, c].astype(F32)).astype(BF16)
        to(tile, cross.at[r, c], sent.at[1], cross_in.at[t], side).start()

    def slot(p, bi, h):
        return total.at[p, pl.ds(pl.multiple_of(bi * RB + h * S, S), S)]

    def step_total(t):
        h = t // F

        @pl.when(lax.rem(t, F) == 0)
        def _():
            own_rows(h).wait()

        i = block(core, t)
        r, c = rows(t), cols(i)
        tile, arrived = half.at[r, c], cross.at[r, c]
        pltpu.make_async_copy(tile, tile, pair_in.at[t]).wait()
        pltpu.make_async_copy(arrived, arrived, cross_in.at[t]).wait()
        tile[...] = (
            tile[...].astype(F32) + out[core, r, c].astype(F32) + arrived[...].astype(F32)
        ).astype(BF16)
        dst, sem = slot(core, b, h), total_in.at[(core * B + b) * H + h]
        here = jnp.logical_and(mine, i == f)

        @pl.when(here)
        def _():
            pltpu.make_async_copy(tile, dst, sem).start()

        @pl.when(jnp.logical_not(here))
        def _():
            to(tile, dst, sent.at[2], sem, (a, i)).start()

    def step_update(t):
        h, k = t // F, lax.rem(t, F)
        for p in range(PROJ):
            e = lax.rem(f + 2 * F - k - p * (F // 2), F)

            @pl.when(e // B == w)
            def _():
                be = lax.rem(e, B)
                tile = slot(p, be, h)
                pltpu.make_async_copy(tile, tile, total_in.at[(p * B + be) * H + h]).wait()
                rr = pl.ds(pl.multiple_of(be * RB + h * S, S), S)
                outer = tile[...].astype(F32) / R
                velocity = 0.9 * mom[p, rr] + outer
                updated = mas[p, rr] - 0.7 * (outer + 0.9 * velocity)
                mom[p, rr] = velocity
                mas[p, rr] = updated
                tile[...] = updated.astype(BF16)
                dst = out.at[p, rows(t), cols(f)]
                here = jnp.logical_and(mine, jnp.logical_and(p == core, e == f))

                @pl.when(here)
                def _():
                    pltpu.make_async_copy(tile, dst, back_in.at[t]).start()

                @pl.when(jnp.logical_not(here))
                def _():
                    to(tile, dst, sent.at[3], back_in.at[t], (x * PROJ + p, e)).start()

    def step_side(t):
        tile = out.at[core, rows(t), cols(block(core, t))]
        pltpu.make_async_copy(tile, tile, back_in.at[t]).wait()
        to(tile, tile, sent.at[4], side_in.at[t], side).start()
        to(tile, tile, sent.at[5], last_in, pair).start()

    def step_pair(t):
        tile = out.at[core, rows(t), cols(block(core, t))]
        pltpu.make_async_copy(tile, tile, side_in.at[t]).wait()
        to(tile, tile, sent.at[5], last_in, pair).start()

    load_first.wait()

    @pl.loop(0, min(AHEAD, T))
    def _(t):
        send_pair(t)

    load_mas = pltpu.make_async_copy(master, mas, load.at[0])
    load_mom = pltpu.make_async_copy(momentum, mom, load.at[1])

    @pl.loop(0, T + LAGS[-1])
    def _(t):
        @pl.when(t + AHEAD < T)
        def _():
            send_pair(t + AHEAD)

        @pl.when(jnp.logical_and(far, t < T))
        def _():
            step_cross(t)

        @pl.when(t == 0)
        def _():
            load_mas.start()
            load_mom.start()

        @pl.when(t == LAGS[1])
        def _():
            load_mas.wait()
            load_mom.wait()

        def late(lag, on, step):
            @pl.when(jnp.logical_and(on, jnp.logical_and(t >= lag, t < T + lag)))
            def _():
                step(t - lag)

        late(LAGS[0], near, step_total)
        late(LAGS[1], True, step_update)
        late(LAGS[2], near, step_side)
        late(LAGS[3], far, step_pair)

    drain(out.at[other], last_in)
    drain(half, sent.at[0])
    drain(half, sent.at[5])

    def drain_blocks(n, sem):
        drain(half.at[pl.ds(0, RB), pl.ds(0, n * WD)], sem)

    @pl.when(far)
    def _():
        drain_blocks(F, sent.at[1])
        drain_blocks(PROJ * B, sent.at[3])

    @pl.when(near)
    def _():
        drain_blocks(F, sent.at[4])

    @pl.when(mine)
    def _():
        drain_blocks(F - 1, sent.at[2])
        drain_blocks(PROJ * B - 1, sent.at[3])

    @pl.when(jnp.logical_and(near, jnp.logical_not(mine)))
    def _():
        drain_blocks(F, sent.at[2])
        drain_blocks(PROJ * B, sent.at[3])


def store(*refs):
    sources, targets, sem = refs[:3], refs[3:6], refs[6]
    copies = []
    for j, (src, dst) in enumerate(zip(sources, targets)):
        rows = src.shape[1] // PIECES
        for i in range(src.shape[0]):
            for k in range(PIECES):
                r = pl.ds(k * rows, rows)
                copies.append(pltpu.make_async_copy(src.at[i, r], dst.at[i, r], sem.at[j, i, k]))
    for copy in copies:
        copy.start()
    for copy in copies:
        copy.wait()


def on_device(deltas, master, momentum):
    local = deltas[0]
    R, F = lax.axis_size("replica"), lax.axis_size("fsdp")
    PROJ, RB, FF = local.shape
    WD = FF // F
    H = min(SPLITS, RB // 16)
    assert R == 2 * PROJ and PROJ == 2 and F % R == 0 and RB % H == 0 and WD % 128 == 0
    T, B = F * H, F // R
    hbm, vmem = pl.BlockSpec(memory_space=pl.ANY), pl.BlockSpec(memory_space=pltpu.VMEM)
    dma = pltpu.SemaphoreType.DMA
    results = pl.pallas_call(
        functools.partial(kernel, (R, F, PROJ, RB, FF, WD, H)),
        out_shape=(
            pltpu.VMEM(master.shape, F32),
            pltpu.VMEM(momentum.shape, F32),
            pltpu.VMEM(local.shape, BF16),
        ),
        in_specs=[hbm] * 3,
        out_specs=(vmem,) * 3,
        scratch_shapes=[
            pltpu.VMEM((RB, FF), BF16),
            pltpu.VMEM((RB, FF), BF16),
            pltpu.VMEM(master.shape, BF16),
            pltpu.VMEM((RB // H, FF), BF16),
            dma((3,)), dma((H,)), dma((6,)),
            dma((T,)), dma((T,)), dma((PROJ * B * H,)), dma((T,)), dma((T,)), dma,
        ],
        compiler_params=pltpu.CompilerParams(
            collective_id=0, has_side_effects=True, vmem_limit_bytes=24 * 2**20
        ),
    )(local, master, momentum)
    return pl.pallas_call(
        store,
        out_shape=[jax.ShapeDtypeStruct(r.shape, r.dtype) for r in results],
        in_specs=[vmem] * 3,
        out_specs=[hbm] * 3,
        scratch_shapes=[dma((3, PROJ, PIECES))],
        compiler_params=pltpu.CompilerParams(vmem_limit_bytes=2**20),
    )(*(pltpu.with_memory_space_constraint(r, pltpu.VMEM) for r in results))


def solution(mesh):
    return jax.shard_map(
        on_device,
        mesh=mesh,
        in_specs=(
            P("replica", None, "fsdp", None),
            P(None, "replica", "fsdp"),
            P(None, "replica", "fsdp"),
        ),
        out_specs=(P(None, "replica", "fsdp"), P(None, "replica", "fsdp"), P(None, "fsdp", None)),
        check_vma=False,
    )
```

```python
import functools

import jax
import jax.numpy as jnp
from jax import lax
from jax.experimental import pallas as pl
from jax.experimental.pallas import tpu as pltpu
from jax.sharding import PartitionSpec as P

F32, BF16 = jnp.float32, jnp.bfloat16
SPLITS = 16
AHEAD = 8
PIECES = 4
CATCH = 3
LAGS = (6, 10, 14, 18)


def kernel(
    dims, delta, master, momentum, mas, mom, out,
    half, cross, total, first,
    load, load_own, sent, pair_in, cross_in, total_in, back_in, side_in, last_in,
):
    R, F, PROJ, RB, FF, WD, H = dims
    B, S, T = F // R, RB // H, F * H
    w, f = lax.axis_index("replica"), lax.axis_index("fsdp")
    core, x = lax.rem(w, PROJ), w // PROJ
    a, b = f // B, lax.rem(f, B)
    other = 1 - core
    pair = (x * PROJ + other, f)
    side = ((1 - x) * PROJ + core, f)
    near = x == a // PROJ
    far = jnp.logical_not(near)
    mine = a == w

    def to(ref_src, ref_dst, send, recv, device):
        return pltpu.make_async_remote_copy(
            src_ref=ref_src, dst_ref=ref_dst, send_sem=send, recv_sem=recv,
            device_id=device, device_id_type=pl.DeviceIdType.MESH,
        )

    def drain(ref, sem):
        pltpu.make_async_copy(ref, ref, sem).wait()

    def block(c, t):
        return lax.rem(lax.rem(t, F) + f + c * (F // 2), F)

    def rows(t):
        return pl.ds(pl.multiple_of((t // F) * S, S), S)

    def cols(i):
        return pl.ds(pl.multiple_of(i * WD, 128), WD)

    def own_rows(h):
        r = pl.ds(pl.multiple_of(h * S, S), S)
        return pltpu.make_async_copy(delta.at[core, r], out.at[core, r], load_own.at[h])

    load_first = pltpu.make_async_copy(delta.at[other, pl.ds(0, S)], first, load.at[2])
    load_first.start()
    barrier = pltpu.get_barrier_semaphore()

    def greet(device):
        pl.semaphore_signal(barrier, inc=1, device_id=device, device_id_type=pl.DeviceIdType.MESH)

    greet(pair)
    greet(side)

    @pl.loop(0, PROJ * B)
    def _(i):
        p, bi = i // B, lax.rem(i, B)

        @pl.when(jnp.logical_not(jnp.logical_and(mine, jnp.logical_and(p == core, bi == b))))
        def _():
            greet((x * PROJ + p, w * B + bi))

    @pl.when(near)
    def _():
        @pl.loop(0, F)
        def _(i):
            @pl.when(jnp.logical_not(jnp.logical_and(mine, i == f)))
            def _():
                greet((a, i))

    @pl.loop(0, H)
    def _(h):
        own_rows(h).start()

    @pl.when(far)
    def _():
        pl.semaphore_wait(barrier, 2 + PROJ * B)

    @pl.when(mine)
    def _():
        pl.semaphore_wait(barrier, PROJ * B + F)

    @pl.when(jnp.logical_and(near, jnp.logical_not(mine)))
    def _():
        pl.semaphore_wait(barrier, 2 + PROJ * B + F)

    def send_pair(t):
        c = cols(block(other, t))
        dst, sem = half.at[rows(t), c], pair_in.at[t]

        @pl.when(t < F)
        def _():
            to(first.at[:, c], dst, sent.at[0], sem, pair).start()

        @pl.when(t >= F)
        def _():
            to(delta.at[other, rows(t), c], dst, sent.at[0], sem, pair).start()

    def step_cross(t):
        @pl.when(lax.rem(t, F) == 0)
        def _():
            own_rows(t // F).wait()

        r, c = rows(t), cols(block(core, t))
        tile = half.at[r, c]
        pltpu.make_async_copy(tile, tile, pair_in.at[t]).wait()
        tile[...] = (tile[...].astype(F32) + out[core, r, c].astype(F32)).astype(BF16)
        to(tile, cross.at[r, c], sent.at[1], cross_in.at[t], side).start()

    def slot(p, bi, h):
        return total.at[p, pl.ds(pl.multiple_of(bi * RB + h * S, S), S)]

    def step_total(t):
        h = t // F

        @pl.when(lax.rem(t, F) == 0)
        def _():
            own_rows(h).wait()

        i = block(core, t)
        r, c = rows(t), cols(i)
        tile, arrived = half.at[r, c], cross.at[r, c]
        pltpu.make_async_copy(tile, tile, pair_in.at[t]).wait()
        pltpu.make_async_copy(arrived, arrived, cross_in.at[t]).wait()
        tile[...] = (
            tile[...].astype(F32) + out[core, r, c].astype(F32) + arrived[...].astype(F32)
        ).astype(BF16)
        dst, sem = slot(core, b, h), total_in.at[(core * B + b) * H + h]
        here = jnp.logical_and(mine, i == f)

        @pl.when(here)
        def _():
            pltpu.make_async_copy(tile, dst, sem).start()

        @pl.when(jnp.logical_not(here))
        def _():
            to(tile, dst, sent.at[2], sem, (a, i)).start()

    def step_update(t):
        h, k = t // F, lax.rem(t, F)
        for p in range(PROJ):
            e = lax.rem(f + 2 * F - k - p * (F // 2), F)

            @pl.when(e // B == w)
            def _():
                be = lax.rem(e, B)
                tile = slot(p, be, h)
                pltpu.make_async_copy(tile, tile, total_in.at[(p * B + be) * H + h]).wait()
                rr = pl.ds(pl.multiple_of(be * RB + h * S, S), S)
                outer = tile[...].astype(F32) / R
                velocity = 0.9 * mom[p, rr] + outer
                updated = mas[p, rr] - 0.7 * (outer + 0.9 * velocity)
                mom[p, rr] = velocity
                mas[p, rr] = updated
                tile[...] = updated.astype(BF16)
                dst = out.at[p, rows(t), cols(f)]
                here = jnp.logical_and(mine, jnp.logical_and(p == core, e == f))

                @pl.when(here)
                def _():
                    pltpu.make_async_copy(tile, dst, back_in.at[t]).start()

                @pl.when(jnp.logical_not(here))
                def _():
                    to(tile, dst, sent.at[3], back_in.at[t], (x * PROJ + p, e)).start()

    def step_side(t):
        tile = out.at[core, rows(t), cols(block(core, t))]
        pltpu.make_async_copy(tile, tile, back_in.at[t]).wait()
        to(tile, tile, sent.at[4], side_in.at[t], side).start()
        to(tile, tile, sent.at[5], last_in, pair).start()

    def step_pair(t):
        tile = out.at[core, rows(t), cols(block(core, t))]
        pltpu.make_async_copy(tile, tile, side_in.at[t]).wait()
        to(tile, tile, sent.at[5], last_in, pair).start()

    load_first.wait()

    @pl.loop(0, min(AHEAD, T))
    def _(t):
        send_pair(t)

    load_mas = pltpu.make_async_copy(master, mas, load.at[0])
    load_mom = pltpu.make_async_copy(momentum, mom, load.at[1])

    @pl.loop(0, T + LAGS[-1])
    def _(t):
        @pl.when(t + AHEAD < T)
        def _():
            send_pair(t + AHEAD)

        @pl.when(jnp.logical_and(far, t < T))
        def _():
            step_cross(t)

        @pl.when(t == 0)
        def _():
            load_mas.start()
            load_mom.start()

        @pl.when(t == LAGS[1])
        def _():
            load_mas.wait()
            load_mom.wait()

        catch = min(CATCH, T // 2)

        def late(lag, on, step):
            @pl.when(jnp.logical_and(on, jnp.logical_and(t >= lag, t < T + lag)))
            def _():
                step(t - lag)

        late(LAGS[0], near, step_total)
        late(LAGS[1], True, step_update)
        begun = t - (T + LAGS[0] - catch)
        late(LAGS[2] - jnp.clip(begun, 0, catch), near, step_side)
        late(LAGS[2] - jnp.clip(begun, 0, catch) - 1, jnp.logical_and(near, jnp.logical_and(begun >= 0, begun < catch)), step_side)
        late(LAGS[3], far, step_pair)

    drain(out.at[other], last_in)
    drain(half, sent.at[0])
    drain(half, sent.at[5])

    def drain_blocks(n, sem):
        drain(half.at[pl.ds(0, RB), pl.ds(0, n * WD)], sem)

    @pl.when(far)
    def _():
        drain_blocks(F, sent.at[1])
        drain_blocks(PROJ * B, sent.at[3])

    @pl.when(near)
    def _():
        drain_blocks(F, sent.at[4])

    @pl.when(mine)
    def _():
        drain_blocks(F - 1, sent.at[2])
        drain_blocks(PROJ * B - 1, sent.at[3])

    @pl.when(jnp.logical_and(near, jnp.logical_not(mine)))
    def _():
        drain_blocks(F, sent.at[2])
        drain_blocks(PROJ * B, sent.at[3])


def store(*refs):
    sources, targets, sem = refs[:3], refs[3:6], refs[6]
    copies = []
    for j, (src, dst) in enumerate(zip(sources, targets)):
        rows = src.shape[1] // PIECES
        for i in range(src.shape[0]):
            for k in range(PIECES):
                r = pl.ds(k * rows, rows)
                copies.append(pltpu.make_async_copy(src.at[i, r], dst.at[i, r], sem.at[j, i, k]))
    for copy in copies:
        copy.start()
    for copy in copies:
        copy.wait()


def on_device(deltas, master, momentum):
    local = deltas[0]
    R, F = lax.axis_size("replica"), lax.axis_size("fsdp")
    PROJ, RB, FF = local.shape
    WD = FF // F
    H = min(SPLITS, RB // 16)
    assert R == 2 * PROJ and PROJ == 2 and F % R == 0 and RB % H == 0 and WD % 128 == 0
    T, B = F * H, F // R
    hbm, vmem = pl.BlockSpec(memory_space=pl.ANY), pl.BlockSpec(memory_space=pltpu.VMEM)
    dma = pltpu.SemaphoreType.DMA
    results = pl.pallas_call(
        functools.partial(kernel, (R, F, PROJ, RB, FF, WD, H)),
        out_shape=(
            pltpu.VMEM(master.shape, F32),
            pltpu.VMEM(momentum.shape, F32),
            pltpu.VMEM(local.shape, BF16),
        ),
        in_specs=[hbm] * 3,
        out_specs=(vmem,) * 3,
        scratch_shapes=[
            pltpu.VMEM((RB, FF), BF16),
            pltpu.VMEM((RB, FF), BF16),
            pltpu.VMEM(master.shape, BF16),
            pltpu.VMEM((RB // H, FF), BF16),
            dma((3,)), dma((H,)), dma((6,)),
            dma((T,)), dma((T,)), dma((PROJ * B * H,)), dma((T,)), dma((T,)), dma,
        ],
        compiler_params=pltpu.CompilerParams(
            collective_id=0, has_side_effects=True, vmem_limit_bytes=24 * 2**20
        ),
    )(local, master, momentum)
    return pl.pallas_call(
        store,
        out_shape=[jax.ShapeDtypeStruct(r.shape, r.dtype) for r in results],
        in_specs=[vmem] * 3,
        out_specs=[hbm] * 3,
        scratch_shapes=[dma((3, PROJ, PIECES))],
        compiler_params=pltpu.CompilerParams(vmem_limit_bytes=2**20),
    )(*(pltpu.with_memory_space_constraint(r, pltpu.VMEM) for r in results))


def solution(mesh):
    return jax.shard_map(
        on_device,
        mesh=mesh,
        in_specs=(
            P("replica", None, "fsdp", None),
            P(None, "replica", "fsdp"),
            P(None, "replica", "fsdp"),
        ),
        out_specs=(P(None, "replica", "fsdp"), P(None, "replica", "fsdp"), P(None, "fsdp", None)),
        check_vma=False,
    )
```
